32 devices in a mesh: section: 4 (over z), col: 8 (over y, x, core).
Axes of the slice: x: 2, y: 2, z: 4, core: 2. Of those that a mesh axis runs over, the one named last changes fastest.
Arguments:
- tiles: bfloat16 [256, 12, 128, 128], P('col', None, 'section'), may hold values from 0.0099487305 to 1
- offsets: int32 [256, 12], replicated, may hold values from -6 to 6, as said below
- counts: int32 [256], replicated, may hold values from 1 to 12
- ranks: int32 [256, 25, 128, 128], P('col', None, 'section'), may hold values from 0 to 3199, as said below
Outputs:
- pruned: bfloat16 [256, 25, 128, 128], P('col', None, 'section')
The draws below stay inside these ranges and needn't reach their ends.
Inputs may be any that keep to these rules, and one draw needn't show every extreme that they name: Within each panel the 12 offsets are distinct, each from -6 to 6. For every panel j and column c, ranks[j, :, c, :] holds each of 0 .. 3199 once.
All inputs are finite; a program needn't handle non-finite values.
Results may differ from the reference program's by a relative error of at most 0.001.
Values may be sent and summed in bfloat16 or wider, within the bound.
A program may use at most 128 MiB of HBM per device.

```python
import math
import jax
import jax.numpy as jnp
from jax import lax

TILE = 128
KB = 12
W = 6
TOPK = 256
NB = 256
OB = 25


def draw_offsets(key, part):
    keys = jax.random.split(key, NB)
    perms = jax.vmap(lambda single: jax.random.permutation(single, 2 * W + 1))(keys)
    return (perms[:, :KB] - W).astype(jnp.int32)


def draw_ranks(key, part):
    keys = jax.random.split(key, NB * TILE)
    perms = jax.vmap(lambda single: jax.random.permutation(single, OB * TILE))(keys)
    return perms.reshape(NB, TILE, OB, TILE).transpose(0, 2, 1, 3).astype(jnp.int32)


def place_ends(array, rng, least, largest):
    longest = array.shape.index(max(array.shape))
    spots = []
    for shift in (0, 1):
        where = [jax.random.randint(jax.random.fold_in(rng, axis), (), 0, length) for axis, length in enumerate(array.shape)]
        where[longest] = (where[longest] + shift) % array.shape[longest]
        spots.append(tuple(where))
    return array.at[spots[0]].set(least).at[spots[1]].set(largest)


def levels(stream_key, shape, pieces, least, high):
    def one(position, shards_of):
        heights = jax.random.uniform(jax.random.fold_in(jax.random.fold_in(stream_key, 6), position), (shards_of,), jnp.float32, least / len(pieces), high / len(pieces))
        return jnp.repeat(jnp.exp(heights), shape[position] // shards_of).reshape((-1,) + (1,) * (len(shape) - position - 1))

    factor_of = one(*pieces[0])
    for cut in pieces[1:]:
        factor_of = factor_of * one(*cut)
    return factor_of


def setup_inputs(seed: int = 0) -> dict:
    key_of = jax.random.split(jax.random.key(seed), 5)
    tiles = jnp.clip(jnp.exp(math.log(1.0) - 4.61031033 * jax.random.uniform(key_of[0], (NB, KB, TILE, TILE), jnp.float32) ** levels(key_of[0], (NB, KB, TILE, TILE), ((0, 8), (2, 4)), -0.2, 0.2)), 0.0099487305, 1.0).astype(jnp.bfloat16)
    offsets = draw_offsets(jax.random.fold_in(key_of[4], 71), 0)
    counts = place_ends(jax.random.randint(key_of[2], (NB,), 1, KB + 1), jax.random.fold_in(key_of[2], 1), 1, KB).astype(jnp.int32)
    ranks = draw_ranks(jax.random.fold_in(key_of[4], 71), 0)
    return {"tiles": tiles, "offsets": offsets, "counts": counts, "ranks": ranks}


def reference(tiles, offsets, counts, ranks):
    total = tiles.shape[0]
    slots = tiles.shape[1]
    bands = 4 * W + 1
    padded = jnp.pad(tiles, ((W, W), (0, 0), (0, 0), (0, 0)))
    pad_off = jnp.pad(offsets, ((W, W), (0, 0)))
    pad_cnt = jnp.pad(counts, ((W, W),))
    slot_ids = jnp.arange(slots, dtype=jnp.int32)

    def one_panel(panel):
        own = lax.dynamic_index_in_dim(tiles, panel, 0, False).astype(jnp.float32)
        own_off = lax.dynamic_index_in_dim(offsets, panel, 0, False)
        own_cnt = lax.dynamic_index_in_dim(counts, panel, 0, False)
        where_at = (panel + W + own_off).astype(jnp.int32)
        firsts = padded[where_at].astype(jnp.float32)
        first_off = pad_off[where_at]
        first_cnt = pad_cnt[where_at]
        row_own = panel + own_off
        ok_own = (slot_ids < own_cnt) & (row_own >= 0) & (row_own < total)
        row_first = row_own[:, None] + first_off
        ok_first = (slot_ids[None, :] < first_cnt[:, None]) & (row_first >= 0) & (row_first < total)
        weight = (ok_own[:, None] & ok_first).astype(jnp.float32)
        target = own_off[:, None] + first_off + 2 * W
        place = (jnp.arange(bands, dtype=jnp.int32)[:, None, None] == target[None]).astype(jnp.float32) * weight[None]
        products = jnp.einsum('kcx,klxr->klcr', own, firsts, precision=lax.Precision.HIGHEST)
        expanded = jnp.einsum('okl,klcr->ocr', place, products, precision=lax.Precision.HIGHEST)
        keep = lax.dynamic_index_in_dim(ranks, panel, 0, False) < TOPK
        squared = jnp.where(keep, expanded * expanded, jnp.float32(0.0))
        totals = jnp.sum(squared, axis=(0, 2), keepdims=True)
        return (TOPK * squared / (totals + 1e-6)).astype(jnp.bfloat16)

    return lax.map(one_panel, jnp.arange(total, dtype=jnp.int32))
```

```python
import functools

import jax
import jax.numpy as jnp
from jax import lax
from jax.experimental import pallas as pl
from jax.experimental.pallas import tpu as pltpu
from jax.sharding import PartitionSpec as P

W = 6
TOPK = 256
PAIRS = 24
LOAD = 48
BLOCK = 4
ABSENT = 99
MESH = pl.DeviceIdType.MESH


def gather_kernel(chunks, cap, ids, tiles, out, pack, recv_z, recv_p, recv_h, send_d, send_u, send_p, send_h, local):
    size = lax.axis_size("section")
    groups = lax.axis_size("col")
    z = lax.axis_index("section")
    g = lax.axis_index("col")
    odd = g % 2
    partner = g + 1 - 2 * odd
    outer = g - 1 + 2 * odd
    has_outer = (outer >= 0) & (outer < groups)
    halo = chunks[0][1]
    has_down = z >= 1
    has_up = z < size - 1

    barrier = pltpu.get_barrier_semaphore()

    def greet(target):
        pl.semaphore_signal(barrier, inc=1, device_id=target, device_id_type=MESH)

    def down_to(src, c, s):
        at, n = chunks[c]
        return pltpu.make_async_remote_copy(
            src_ref=src, dst_ref=out.at[pl.ds(at, n), s], send_sem=send_d.at[s, c], recv_sem=recv_z.at[s, c],
            device_id={"section": z - 1}, device_id_type=MESH)

    def up_to(src, c, s):
        at, n = chunks[c]
        return pltpu.make_async_remote_copy(
            src_ref=src, dst_ref=out.at[pl.ds(at, n), s], send_sem=send_u.at[s, c], recv_sem=recv_z.at[s, c],
            device_id={"section": z + 1}, device_id_type=MESH)

    def share(src, c, s):
        at, n = chunks[c]
        return pltpu.make_async_remote_copy(
            src_ref=src, dst_ref=out.at[pl.ds(cap + at, n), s], send_sem=send_p.at[s, c], recv_sem=recv_p.at[s, c],
            device_id={"col": partner}, device_id_type=MESH)

    def edge(src, s):
        return pltpu.make_async_remote_copy(
            src_ref=src, dst_ref=out.at[pl.ds(2 * cap, halo), s], send_sem=send_h.at[s], recv_sem=recv_h.at[s],
            device_id={"col": outer}, device_id_type=MESH)

    def keep(c):
        at, n = chunks[c]
        return pltpu.make_async_copy(pack.at[pl.ds(at, n)], out.at[pl.ds(at, n), z], local.at[c])

    def landed(c, s):
        at, n = chunks[c]
        return out.at[pl.ds(at, n), s]

    def fill(c):
        at, n = chunks[c]

        def body(t, carry):
            pack[t] = tiles[ids[t]]
            return carry

        lax.fori_loop(at, at + n, body, 0, unroll=4)

    def send_own(c):
        at, n = chunks[c]
        src = pack.at[pl.ds(at, n)]
        pl.when(has_down)(lambda: down_to(src, c, z).start())
        pl.when(has_up)(lambda: up_to(src, c, z).start())
        share(src, c, z).start()
        if c == 0:
            pl.when(has_outer)(lambda: edge(src, z).start())
        keep(c).start()

    pl.when(has_down)(lambda: greet({"section": z - 1}))
    pl.when(has_up)(lambda: greet({"section": z + 1}))
    greet({"col": partner})
    pl.when(has_outer)(lambda: greet({"col": outer}))
    fill(0)
    expected = 1 + has_down.astype(jnp.int32) + has_up.astype(jnp.int32) + has_outer.astype(jnp.int32)
    pl.semaphore_wait(barrier, expected)
    count = len(chunks)
    for c in range(1, count):
        fill(c)
        send_own(c - 1)
    send_own(count - 1)

    def arrived(c, s):
        at, n = chunks[c]
        src = landed(c, s)
        share(src, c, s).start()
        if c == 0:
            pl.when(has_outer)(lambda: edge(src, s).start())

    for d in range(1, size):
        for c in range(count):
            above = z + d
            below = z - d

            @pl.when(above < size)
            def _():
                up_to(landed(c, above), c, above).wait_recv()
                pl.when(has_down)(lambda: down_to(landed(c, above), c, above).start())
                arrived(c, above)

            @pl.when(below >= 0)
            def _():
                down_to(landed(c, below), c, below).wait_recv()
                pl.when(has_up)(lambda: up_to(landed(c, below), c, below).start())
                arrived(c, below)

    for s in range(size):
        for c in range(count):
            share(landed(c, s), c, s).wait()
            pl.when(has_down & (s >= z))(lambda: down_to(landed(c, s), c, s).wait_send())
            pl.when(has_up & (s <= z))(lambda: up_to(landed(c, s), c, s).wait_send())
        pl.when(has_outer)(lambda: edge(landed(0, s), s).wait())
    for c in range(count):
        keep(c).wait()


def run_gather(level, chunks, cap, ids, tiles):
    full, columns, rows = tiles.shape
    size = lax.axis_size("section")
    count = len(chunks)
    total = 2 * cap + chunks[0][1]
    dma = pltpu.SemaphoreType.DMA
    return pl.pallas_call(
        functools.partial(gather_kernel, chunks, cap),
        in_specs=[pl.BlockSpec(memory_space=pltpu.SMEM), pl.BlockSpec(memory_space=pltpu.VMEM)],
        out_specs=pl.BlockSpec(memory_space=pl.ANY),
        out_shape=jax.ShapeDtypeStruct((total, size, columns, rows), tiles.dtype),
        scratch_shapes=[
            pltpu.VMEM((cap, columns, rows), tiles.dtype),
            dma((size, count)), dma((size, count)), dma((size,)),
            dma((size, count)), dma((size, count)), dma((size, count)), dma((size,)), dma((count,)),
        ],
        compiler_params=pltpu.CompilerParams(collective_id=level, has_side_effects=True),
    )(ids, tiles)


def plan_kernel(caps, bands, sums, near, ids, entries, first, need, counted, started, offset_of, slot_of):
    window, slots = near.shape
    panels = window - 2 * W
    g = lax.axis_index("col")
    odd = g % 2
    sign = 1 - 2 * odd
    half = (slots + 1) // 2

    def most(i, value):
        return jnp.maximum(value, sums[i])

    needed = lax.fori_loop(0, sums.shape[0], most, 0)
    cap = jnp.int32(caps[0])
    for level in range(1, len(caps)):
        cap = jnp.where(needed > caps[level - 1], caps[level], cap)
    partner_total = sums[g + 1 - 2 * odd]

    def scan_panel(n, at, own):
        real = jnp.where(odd == 1, window - 1 - n, n)
        started[n] = at
        here = jnp.int32(0)
        for s in range(slots):
            value = near[real, s]
            offset_of[n * slots + here] = value
            slot_of[n * slots + here] = s
            if own:
                ids[at + here] = (real - W) * slots + s
            here = here + jnp.where(value < ABSENT, 1, 0)
        counted[n] = here
        return at + here

    def outer(i, at):
        return scan_panel(W - 1 - i, at, False)

    def mine(i, at):
        return scan_panel(W + i, at, True)

    def beyond(i, at):
        return scan_panel(window - 1 - i, at, False)

    lax.fori_loop(0, W, outer, 2 * cap)
    own_total = lax.fori_loop(0, panels, mine, jnp.int32(0))

    def blank(i, carry):
        ids[i] = 0
        return carry

    lax.fori_loop(own_total, ids.shape[0], blank, 0)

    def tally(i, value):
        n = window - 1 - i
        real = jnp.where(odd == 1, window - 1 - n, n)
        for s in range(slots):
            value = value + jnp.where(near[real, s] < ABSENT, 1, 0)
        return value

    edge_total = lax.fori_loop(0, W, tally, jnp.int32(0))
    lax.fori_loop(0, W, beyond, cap + partner_total - edge_total)

    blocks = panels // BLOCK
    empty = (bands << 16) + (bands << 23)

    def one_block(b, at):
        first[b] = at // PAIRS

        def one_panel(i, at):
            n = W + b * BLOCK + i
            spot = jnp.where(odd == 1, BLOCK - 1 - i, i)
            row = spot * (bands + 1)

            def one_slot(k, at):
                off = offset_of[n * slots + k]
                m = n + sign * off
                count = counted[m]
                source = started[m]
                base = spot * slots + slot_of[n * slots + k] + (source << 6)
                target = row + off + 2 * W
                for h in range(half):
                    one = target + offset_of[m * slots + 2 * h]
                    two = target + offset_of[m * slots + min(2 * h + 1, slots - 1)]
                    two = jnp.where(count > 2 * h + 1, two, row + bands)
                    entries[at + h] = base + (2 * h << 6) + (one << 16) + (two << 23)
                return at + ((count + 1) >> 1)

            return lax.fori_loop(0, counted[n], one_slot, at)

        at = lax.fori_loop(0, BLOCK, one_panel, at)
        for i in range(PAIRS):
            entries[at + i] = empty
        n = W + b * BLOCK + BLOCK - 1 + W
        last = jnp.minimum(n, W + panels - 1)
        end = started[last] + counted[last]
        need[b + 1] = jnp.where(n > last, 9999, 1 + (end + LOAD - 1) // LOAD)
        return (at + PAIRS - 1) // PAIRS * PAIRS

    need[0] = 0
    end = lax.fori_loop(0, blocks, one_block, jnp.int32(0))
    first[blocks] = end // PAIRS


def run_plan(caps, bands, sums, near):
    window, slots = near.shape
    panels = window - 2 * W
    blocks = panels // BLOCK
    span = panels * slots * ((slots + 1) // 2) + (blocks + 1) * PAIRS + slots
    smem = pl.BlockSpec(memory_space=pltpu.SMEM)
    one = lambda n: jax.ShapeDtypeStruct((n,), jnp.int32)
    return pl.pallas_call(
        functools.partial(plan_kernel, caps, bands),
        in_specs=[smem, smem],
        out_specs=[smem] * 4,
        out_shape=[one(panels * slots + slots), one(span), one(blocks + 1), one(blocks + 1)],
        scratch_shapes=[
            pltpu.SMEM((window,), jnp.int32), pltpu.SMEM((window,), jnp.int32),
            pltpu.SMEM((window * slots + slots,), jnp.int32), pltpu.SMEM((window * slots + slots,), jnp.int32),
        ],
    )(sums, near)


def panel_kernel(bands, loads, first, need, entries, band_hbm, own_ref, ranks_ref, out_ref, band, acc, sems):
    step = pl.program_id(0)

    def load(i):
        at, n = loads[i]
        return pltpu.make_async_copy(band_hbm.at[pl.ds(at, n)], band.at[pl.ds(at, n)], sems.at[i])

    @pl.when(step == 0)
    def _():
        for i in range(len(loads)):
            load(i).start()
        acc[...] = jnp.zeros_like(acc)

    before = need[step]
    after = need[step + 1]
    for i in range(len(loads)):
        pl.when((before <= i) & (i < after))(lambda: load(i).wait())

    slots = own_ref.shape[1]

    def one_group(q, carry):
        base = q * PAIRS
        for i in range(PAIRS):
            entry = entries[base + i]
            slot = entry & 63
            at = (entry >> 6) & 1023
            one = (entry >> 16) & 127
            two = (entry >> 23) & 127
            lhs = own_ref[slot]
            rhs = jnp.concatenate([band[at], band[at + 1]], axis=1)
            product = jnp.dot(lhs, rhs, preferred_element_type=jnp.float32)
            half = product.shape[1] // 2
            acc[one] += product[:, :half]
            acc[two] += product[:, half:]
        return carry

    lax.fori_loop(first[step], first[step + 1], one_group, 0)

    for b in range(BLOCK):
        row = b * (bands + 1)
        total = jnp.zeros(acc.shape[1:], jnp.float32)
        for o in range(bands):
            value = acc[row + o]
            total = total + jnp.where(ranks_ref[b, o] < TOPK, value * value, 0.0)
        totals = jnp.sum(total, axis=1, keepdims=True) + 1e-06
        scale = jnp.broadcast_to(TOPK / totals, total.shape)
        for o in range(bands):
            value = acc[row + o]
            squared = jnp.where(ranks_ref[b, o] < TOPK, value * value, 0.0)
            out_ref[b, o] = (squared * scale).astype(out_ref.dtype)
            acc[row + o] = jnp.zeros_like(value)


def run_panels(tables, loads, band, tiles, ranks):
    panels, bands, columns, rows = ranks.shape
    slots = tiles.shape[0] // panels
    total = band.shape[0]
    blocks = panels // BLOCK

    def place(i, *_):
        return jnp.where(lax.axis_index("col") % 2 == 1, blocks - 1 - i, i)

    return pl.pallas_call(
        functools.partial(panel_kernel, bands, loads),
        grid_spec=pltpu.PrefetchScalarGridSpec(
            num_scalar_prefetch=len(tables),
            grid=(blocks,),
            in_specs=[
                pl.BlockSpec(memory_space=pl.ANY),
                pl.BlockSpec((BLOCK * slots, columns, rows), lambda i, *_: (place(i), 0, 0)),
                pl.BlockSpec((BLOCK, bands, columns, rows), lambda i, *_: (place(i), 0, 0, 0)),
            ],
            out_specs=pl.BlockSpec((BLOCK, bands, columns, rows), lambda i, *_: (place(i), 0, 0, 0)),
            scratch_shapes=[
                pltpu.VMEM((total + slots + 1, rows, rows), jnp.bfloat16),
                pltpu.VMEM((BLOCK * (bands + 1), columns, rows), jnp.float32),
                pltpu.SemaphoreType.DMA((len(loads),)),
            ],
        ),
        out_shape=jax.ShapeDtypeStruct(ranks.shape, jnp.bfloat16),
        compiler_params=pltpu.CompilerParams(
            dimension_semantics=("arbitrary",), vmem_limit_bytes=56 * 2**20
        ),
        cost_estimate=pl.CostEstimate(
            flops=panels * 10**8, bytes_accessed=panels * 10**6, transcendentals=0
        ),
    )(*tables, band, tiles, ranks)


def cut(start, stop, piece):
    return [(at, min(piece, stop - at)) for at in range(start, stop, piece)]


def shards(tiles, offsets, counts, ranks):
    panels, slots, columns, rows = tiles.shape
    bands = ranks.shape[1]
    total = offsets.shape[0]
    groups = lax.axis_size("col")
    me = lax.axis_index("col")
    full = panels * slots
    halo = W * slots

    slot_ids = jnp.arange(slots, dtype=jnp.int32)[None]
    row_of = jnp.arange(total, dtype=jnp.int32)[:, None] + offsets
    valid = (slot_ids < counts[:, None]) & (row_of >= 0) & (row_of < total)
    sums = jnp.sum(valid.astype(jnp.int32).reshape(groups, full), axis=1)
    needed = jnp.max(sums)
    coded = jnp.where(valid, offsets, ABSENT)
    coded = jnp.pad(coded, ((W, W), (0, 0)), constant_values=ABSENT)
    near = lax.dynamic_slice_in_dim(coded, me * panels, panels + 2 * W, 0)

    caps = sorted({max(2 * halo, full * part // 48) for part in (28, 29, 30, 31, 33, 36, 48)})
    ids, entries, first, need = run_plan(caps, bands, sums, near)
    flat = tiles.reshape(full, columns, rows)

    def at_capacity(level, cap):
        chunks = [(0, halo)] + cut(halo, cap, -(-(cap - halo) // 4))
        loads = cut(2 * cap, 2 * cap + halo, halo) + cut(0, cap, LOAD) + cut(cap, 2 * cap, LOAD)

        def run():
            band = run_gather(level, chunks, cap, ids, flat)
            band = band.reshape(band.shape[0], rows, rows)
            return run_panels((first, need, entries), loads, band, flat, ranks)
        return run

    which = sum((needed > cap).astype(jnp.int32) for cap in caps[:-1])
    return lax.switch(which, [at_capacity(level, cap) for level, cap in enumerate(caps)])


def solution(mesh):
    placed = (P("col", None, "section", None), P(), P(), P("col", None, "section", None))
    return jax.shard_map(
        shards,
        mesh=mesh,
        in_specs=placed,
        out_specs=P("col", None, "section", None),
        check_vma=False,
    )
```

```python
import functools

import jax
import jax.numpy as jnp
from jax import lax
from jax.experimental import pallas as pl
from jax.experimental.pallas import tpu as pltpu
from jax.sharding import PartitionSpec as P

W = 6
TOPK = 256
PAIRS = 24
LOAD = 48
BLOCK = 4
EXTRA = 48
ABSENT = 99
MESH = pl.DeviceIdType.MESH


def gather_kernel(chunks, cap, full, facts, ids, tiles, out, pack, extra, recv_z, recv_p, recv_h, send_d, send_u, send_p, send_h, local, swap):
    size = lax.axis_size("section")
    groups = lax.axis_size("col")
    z = lax.axis_index("section")
    g = lax.axis_index("col")
    odd = g % 2
    partner = g + 1 - 2 * odd
    outer = g - 1 + 2 * odd
    has_outer = (outer >= 0) & (outer < groups)
    halo = chunks[0][1]
    has_down = z >= 1
    has_up = z < size - 1
    pooled = cap < full

    barrier = pltpu.get_barrier_semaphore()

    def greet(target):
        pl.semaphore_signal(barrier, inc=1, device_id=target, device_id_type=MESH)

    def down_to(src, c, s):
        at, n = chunks[c]
        return pltpu.make_async_remote_copy(
            src_ref=src, dst_ref=out.at[pl.ds(at, n), s], send_sem=send_d.at[s, c], recv_sem=recv_z.at[s, c],
            device_id={"section": z - 1}, device_id_type=MESH)

    def up_to(src, c, s):
        at, n = chunks[c]
        return pltpu.make_async_remote_copy(
            src_ref=src, dst_ref=out.at[pl.ds(at, n), s], send_sem=send_u.at[s, c], recv_sem=recv_z.at[s, c],
            device_id={"section": z + 1}, device_id_type=MESH)

    def share(src, c, s):
        at, n = chunks[c]
        return pltpu.make_async_remote_copy(
            src_ref=src, dst_ref=out.at[pl.ds(full + at, n), s], send_sem=send_p.at[s, c], recv_sem=recv_p.at[s, c],
            device_id={"col": partner}, device_id_type=MESH)

    def edge(src, s):
        return pltpu.make_async_remote_copy(
            src_ref=src, dst_ref=out.at[pl.ds(2 * full, halo), s], send_sem=send_h.at[s], recv_sem=recv_h.at[s],
            device_id={"col": outer}, device_id_type=MESH)

    def keep(c):
        at, n = chunks[c]
        return pltpu.make_async_copy(pack.at[pl.ds(at, n)], out.at[pl.ds(at, n), z], local.at[c])

    def lend():
        return pltpu.make_async_remote_copy(
            src_ref=pack.at[pl.ds(cap, EXTRA)], dst_ref=extra, send_sem=swap.at[0], recv_sem=swap.at[1],
            device_id={"col": partner}, device_id_type=MESH)

    def landed(c, s):
        at, n = chunks[c]
        return out.at[pl.ds(at, n), s]

    def tile_at(t):
        return tiles[jnp.minimum(jnp.maximum(ids[t], 0), full - 1)]

    def fill(at, n):
        def body(t, carry):
            pack[t] = tile_at(t)
            return carry

        lax.fori_loop(at, at + n, body, 0, unroll=4)

    def fill_last(at, n):
        begin = cap - facts[1]

        def body(t, carry):
            borrowed = extra[jnp.minimum(jnp.maximum(t - begin, 0), EXTRA - 1)]
            pack[t] = jnp.where(t >= begin, borrowed, tile_at(t))
            return carry

        lax.fori_loop(at, at + n, body, 0, unroll=4)

    def send_own(c):
        at, n = chunks[c]
        src = pack.at[pl.ds(at, n)]
        pl.when(has_down)(lambda: down_to(src, c, z).start())
        pl.when(has_up)(lambda: up_to(src, c, z).start())
        share(src, c, z).start()
        if c == 0:
            pl.when(has_outer)(lambda: edge(src, z).start())
        keep(c).start()

    pl.when(has_down)(lambda: greet({"section": z - 1}))
    pl.when(has_up)(lambda: greet({"section": z + 1}))
    greet({"col": partner})
    pl.when(has_outer)(lambda: greet({"col": outer}))
    fill(*chunks[0])
    expected = 1 + has_down.astype(jnp.int32) + has_up.astype(jnp.int32) + has_outer.astype(jnp.int32)
    pl.semaphore_wait(barrier, expected)
    count = len(chunks)
    if pooled:
        fill(cap, EXTRA)
    for c in range(1, count):
        if c == count - 1 and pooled:
            lend().wait_recv()
            fill_last(*chunks[c])
        else:
            fill(*chunks[c])
        send_own(c - 1)
        if c == 1 and pooled:
            lend().start()
    send_own(count - 1)

    def arrived(c, s):
        src = landed(c, s)
        share(src, c, s).start()
        if c == 0:
            pl.when(has_outer)(lambda: edge(src, s).start())

    for d in range(1, size):
        for c in range(count):
            above = z + d
            below = z - d

            @pl.when(above < size)
            def _():
                up_to(landed(c, above), c, above).wait_recv()
                pl.when(has_down)(lambda: down_to(landed(c, above), c, above).start())
                arrived(c, above)

            @pl.when(below >= 0)
            def _():
                down_to(landed(c, below), c, below).wait_recv()
                pl.when(has_up)(lambda: up_to(landed(c, below), c, below).start())
                arrived(c, below)

    for s in range(size):
        for c in range(count):
            share(landed(c, s), c, s).wait()
            pl.when(has_down & (s >= z))(lambda: down_to(landed(c, s), c, s).wait_send())
            pl.when(has_up & (s <= z))(lambda: up_to(landed(c, s), c, s).wait_send())
        pl.when(has_outer)(lambda: edge(landed(0, s), s).wait())
    for c in range(count):
        keep(c).wait()
    if pooled:
        lend().wait_send()


def run_gather(level, chunks, cap, facts, ids, tiles):
    full, columns, rows = tiles.shape
    size = lax.axis_size("section")
    count = len(chunks)
    total = 2 * full + chunks[0][1]
    dma = pltpu.SemaphoreType.DMA
    smem = pl.BlockSpec(memory_space=pltpu.SMEM)
    return pl.pallas_call(
        functools.partial(gather_kernel, chunks, cap, full),
        in_specs=[smem, smem, pl.BlockSpec(memory_space=pltpu.VMEM)],
        out_specs=pl.BlockSpec(memory_space=pl.ANY),
        out_shape=jax.ShapeDtypeStruct((total, size, columns, rows), tiles.dtype),
        scratch_shapes=[
            pltpu.VMEM((cap + EXTRA, columns, rows), tiles.dtype),
            pltpu.VMEM((EXTRA, columns, rows), tiles.dtype),
            dma((size, count)), dma((size, count)), dma((size,)),
            dma((size, count)), dma((size, count)), dma((size, count)), dma((size,)), dma((count,)), dma((2,)),
        ],
        compiler_params=pltpu.CompilerParams(collective_id=level, has_side_effects=True),
    )(facts, ids, tiles)


def plan_kernel(caps, bands, coded, count, ids, entries, first, need, shift, facts, which, counted, started, packed):
    slots, total = coded.shape
    groups = lax.axis_size("col")
    panels = total // groups
    window = panels + 2 * W
    full = panels * slots
    g = lax.axis_index("col")
    odd = g % 2
    half = (slots + 1) // 2

    def sum_of(group):
        parts = [count[group * panels + i] for i in range(panels)]
        while len(parts) > 1:
            parts = [sum(parts[i:i + 2]) for i in range(0, len(parts), 2)]
        return parts[0]

    def most(i, value):
        one = sum_of(2 * i)
        two = sum_of(2 * i + 1)
        return jnp.maximum(value, jnp.maximum((one + two + 1) >> 1, jnp.maximum(one, two) - EXTRA))

    needed = lax.fori_loop(0, groups // 2, most, 0)
    cap = jnp.int32(caps[0])
    level = jnp.int32(0)
    for i in range(1, len(caps)):
        larger = needed > caps[i - 1]
        cap = jnp.where(larger, caps[i], cap)
        level = jnp.where(larger, i, level)
    which[0] = level
    partner_total = sum_of(g + 1 - 2 * odd)
    own_over = jnp.maximum(sum_of(g) - cap, 0)
    partner_over = jnp.maximum(partner_total - cap, 0)
    facts[0] = cap
    facts[1] = partner_over
    facts[2] = jnp.where(own_over > 0, cap, full + cap)
    facts[3] = jnp.where(own_over > 0, full - own_over, -full - partner_over)
    facts[4] = jnp.where(own_over > 0, full, 2 * full)

    def real_of(n):
        return jnp.where(odd == 1, window - 1 - n, n)

    def column(real):
        panel = g * panels + real - W
        beyond = (panel < 0) | (panel >= total)
        panel = jnp.minimum(jnp.maximum(panel, 0), total - 1)
        return panel, jnp.where(beyond, ABSENT, 0)

    def scan_panel(real, at, own):
        panel, bias = column(real)
        started[real] = at
        here = at
        for s in range(slots):
            value = coded[s, panel] + bias
            shift[here] = value
            if own:
                ids[here] = (real - W) * slots + s
                packed[here] = ((real - W) * 16 + s) * 16 + value
            here = here + jnp.where(value < ABSENT, 1, 0)
        counted[real] = here - at
        return here

    def tally(i, value):
        panel, bias = column(real_of(window - 1 - i))
        return value + jnp.where(bias == 0, count[panel], 0)

    edge_total = lax.fori_loop(0, W, tally, jnp.int32(0))
    lax.fori_loop(0, panels, lambda i, at: scan_panel(real_of(W + i), at, True), jnp.int32(0))
    lax.fori_loop(0, W, lambda i, at: scan_panel(real_of(window - 1 - i), at, False),
                  full + partner_total - edge_total)
    lax.fori_loop(0, W, lambda i, at: scan_panel(real_of(W - 1 - i), at, False), jnp.int32(2 * full))

    blocks = panels // BLOCK
    missing = 1 << 23
    empty = (1 << 24) + missing

    def one_block(b, carry):
        u, at = carry
        first[b] = at // PAIRS
        stop = u
        for i in range(BLOCK):
            stop = stop + counted[real_of(W + b * BLOCK + i)]

        def one_tile(u, at):
            code = packed[u]
            off = code & 15
            slot = (code >> 4) & 15
            panel = code >> 8
            source = panel + off
            number = counted[source]
            spot = panel & (BLOCK - 1)
            base = spot * slots + slot + (started[source] << 6) + ((spot * (bands + 1) + off) << 16)
            for h in range(half):
                entries[at + h] = base + (2 * h << 6)
            pairs = (number + 1) >> 1
            last = jnp.maximum(pairs - 1, 0)
            entries[at + last] = base + (last << 7) + ((number & 1) << 23)
            return at + pairs

        at = lax.fori_loop(u, stop, one_tile, at)
        for i in range(PAIRS):
            entries[at + i] = empty
        need[b + 1] = jnp.where(stop > cap, 9999, 1 + (stop + LOAD - 1) // LOAD)
        return stop, (at + PAIRS - 1) // PAIRS * PAIRS

    need[0] = 0
    _, end = lax.fori_loop(0, blocks, one_block, (jnp.int32(0), jnp.int32(0)))
    first[blocks] = end // PAIRS

    def widen(b, carry):
        ahead = (W + BLOCK - 1) // BLOCK
        within = need[jnp.minimum(b + 1 + ahead, blocks)]
        need[b + 1] = jnp.where((b + 1) * BLOCK + W > panels, 9999, within)
        return carry

    lax.fori_loop(0, blocks, widen, 0)


def run_plan(caps, bands, halo, coded, count):
    slots, total = coded.shape
    panels = total // lax.axis_size("col")
    window = panels + 2 * W
    blocks = panels // BLOCK
    full = panels * slots
    span = full * ((slots + 1) // 2) + (blocks + 1) * PAIRS + slots
    smem = pl.BlockSpec(memory_space=pltpu.SMEM)
    one = lambda n: jax.ShapeDtypeStruct((n,), jnp.int32)
    return pl.pallas_call(
        functools.partial(plan_kernel, caps, bands),
        in_specs=[smem, smem],
        out_specs=[smem] * 7,
        out_shape=[one(full + EXTRA + slots), one(span), one(blocks + 1), one(blocks + 1), one(2 * full + halo + slots), one(8), one(1)],
        scratch_shapes=[
            pltpu.SMEM((window,), jnp.int32), pltpu.SMEM((window,), jnp.int32), pltpu.SMEM((full + slots,), jnp.int32),
        ],
    )(coded, count)


def panel_kernel(bands, full, loads, first, need, entries, shift, facts, band_hbm, own_ref, ranks_ref, out_ref, band, acc, sems):
    step = pl.program_id(0)
    cap = facts[0]

    def used(i):
        at, n = loads[i]
        return True if at >= 2 * full else (at % full) < cap

    def load(i):
        at, n = loads[i]
        return pltpu.make_async_copy(band_hbm.at[pl.ds(at, n)], band.at[pl.ds(at, n)], sems.at[i])

    @pl.when(step == 0)
    def _():
        for i in range(len(loads)):
            pl.when(used(i))(lambda: load(i).start())
        acc[...] = jnp.zeros_like(acc)

    before = need[step]
    after = need[step + 1]
    for i in range(len(loads)):
        pl.when((before <= i) & (i < after) & used(i))(lambda: load(i).wait())

    low = facts[2]
    move = facts[3]
    high = facts[4]

    def real(at):
        return at + jnp.where((at >= low) & (at < high), move, 0)

    def one_group(q, carry):
        base = q * PAIRS
        for i in range(PAIRS):
            entry = entries[base + i]
            slot = entry & 63
            at = (entry >> 6) & 1023
            target = (entry >> 16) & 127
            one = jnp.where((entry >> 24) == 0, target + shift[at], bands)
            two = jnp.where(((entry >> 23) & 1) == 0, target + shift[at + 1], bands)
            lhs = own_ref[slot]
            rhs = jnp.concatenate([band[real(at)], band[real(at + 1)]], axis=1)
            product = jnp.dot(lhs, rhs, preferred_element_type=jnp.float32)
            half = product.shape[1] // 2
            acc[one] += product[:, :half]
            acc[two] += product[:, half:]
        return carry

    lax.fori_loop(first[step], first[step + 1], one_group, 0)

    for b in range(BLOCK):
        row = b * (bands + 1)
        total = jnp.zeros(acc.shape[1:], jnp.float32)
        for o in range(bands):
            value = acc[row + o]
            total = total + jnp.where(ranks_ref[b, o] < TOPK, value * value, 0.0)
        totals = jnp.sum(total, axis=1, keepdims=True) + 1e-06
        scale = jnp.broadcast_to(TOPK / totals, total.shape)
        for o in range(bands):
            value = acc[row + o]
            squared = jnp.where(ranks_ref[b, o] < TOPK, value * value, 0.0)
            out_ref[b, o] = (squared * scale).astype(out_ref.dtype)
            acc[row + o] = jnp.zeros_like(value)


def run_panels(tables, loads, band, tiles, ranks):
    panels, bands, columns, rows = ranks.shape
    full = tiles.shape[0]
    slots = full // panels
    total = band.shape[0]
    blocks = panels // BLOCK

    def place(i, *_):
        return jnp.where(lax.axis_index("col") % 2 == 1, blocks - 1 - i, i)

    return pl.pallas_call(
        functools.partial(panel_kernel, bands, full, loads),
        grid_spec=pltpu.PrefetchScalarGridSpec(
            num_scalar_prefetch=len(tables),
            grid=(blocks,),
            in_specs=[
                pl.BlockSpec(memory_space=pl.ANY),
                pl.BlockSpec((BLOCK * slots, columns, rows), lambda i, *_: (place(i), 0, 0)),
                pl.BlockSpec((BLOCK, bands, columns, rows), lambda i, *_: (place(i), 0, 0, 0)),
            ],
            out_specs=pl.BlockSpec((BLOCK, bands, columns, rows), lambda i, *_: (place(i), 0, 0, 0)),
            scratch_shapes=[
                pltpu.VMEM((total + slots + 1, rows, rows), jnp.bfloat16),
                pltpu.VMEM((BLOCK * (bands + 1), columns, rows), jnp.float32),
                pltpu.SemaphoreType.DMA((len(loads),)),
            ],
        ),
        out_shape=jax.ShapeDtypeStruct(ranks.shape, jnp.bfloat16),
        compiler_params=pltpu.CompilerParams(
            dimension_semantics=("arbitrary",), vmem_limit_bytes=56 * 2**20
        ),
        cost_estimate=pl.CostEstimate(
            flops=panels * 10**8, bytes_accessed=panels * 10**6, transcendentals=0
        ),
    )(*tables, band, tiles, ranks)


def cut(start, stop, piece):
    return [(at, min(piece, stop - at)) for at in range(start, stop, piece)]


def shards(tiles, offsets, counts, ranks):
    panels, slots, columns, rows = tiles.shape
    bands = ranks.shape[1]
    total = offsets.shape[0]
    full = panels * slots
    halo = W * slots

    names = offsets.T
    row_of = lax.broadcasted_iota(jnp.int32, names.shape, 1) + names
    slot_ids = lax.broadcasted_iota(jnp.int32, names.shape, 0)
    valid = (slot_ids < counts[None, :]) & (row_of >= 0) & (row_of < total)
    count = jnp.sum(valid.astype(jnp.int32), axis=0)
    coded = jnp.where(valid, names + W, ABSENT)

    least = halo + 2 * EXTRA
    caps = sorted({max(least, full * part // 96) for part in (52, 53, 54, 55, 56, 57, 58, 60, 62, 66, 74)}) + [full]
    ids, entries, first, need, shift, facts, which = run_plan(caps, bands, halo, coded, count)
    flat = tiles.reshape(full, columns, rows)

    def at_capacity(level, cap):
        tail = EXTRA if cap < full else full // 8
        middle = cap - tail - halo
        chunks = [(0, halo)] + cut(halo, cap - tail, -(-middle // 3)) + [(cap - tail, tail)]
        return lambda: run_gather(level, chunks, cap, facts, ids, flat)

    band = lax.switch(which[0], [at_capacity(level, cap) for level, cap in enumerate(caps)])
    band = band.reshape(band.shape[0], rows, rows)
    loads = cut(2 * full, 2 * full + halo, halo) + cut(0, full, LOAD) + cut(full, 2 * full, LOAD)
    return run_panels((first, need, entries, shift, facts), loads, band, flat, ranks)


def solution(mesh):
    placed = (P("col", None, "section", None), P(), P(), P("col", None, "section", None))
    return jax.shard_map(
        shards,
        mesh=mesh,
        in_specs=placed,
        out_specs=P("col", None, "section", None),
        check_vma=False,
    )
```
